32 devices in a mesh: ens: 16 (over z, y, core), batch: 2 (over x).
Axes of the slice: x: 2, y: 2, z: 4, core: 2. Of those that a mesh axis runs over, the one named last changes fastest.
Arguments:
- replay_obs: bfloat16 [512, 1024], P('batch'), may hold values from -4.1875 to 4.1875
- replay_next: bfloat16 [512, 1024], P('batch'), may hold values from -4.1875 to 4.1875
- batch_rows: int32 [64], P('batch'), may hold values from 0 to 255
- data_action: int32 [64], P('batch'), may hold values from 0 to 255
- next_action: int32 [64], P('batch'), may hold values from 0 to 255
- sampled_actions: int32 [64, 16], P('batch'), may hold values from 0 to 255
- reward: float32 [64], P('batch'), may hold values from -6 to 6
- next_logp: float32 [64], P('batch'), may hold values from -6 to 2
- action_table: bfloat16 [256, 1024], replicated, may hold values from -4.1875 to 4.1875
- w1: bfloat16 [16, 4096, 1024], P('ens'), may hold values from -0.1875 to 0.1875
- w2: float32 [16, 4096], P('ens'), may hold values from -0.375 to 0.375
Outputs:
- grad_w1: float32 [16, 4096, 1024], P('ens', 'batch')
- grad_w2: float32 [16, 4096], P('ens')
- critic_stats: float32 [16, 3], P('ens')
The draws below stay inside these ranges and needn't reach their ends.
Inputs may be any that keep to these rules, and one draw needn't show every extreme that they name: `batch_rows`: each entry is a row of the own block of 256 replay rows that holds its state.
All inputs are finite; a program needn't handle non-finite values.
Results may differ from the reference program's by a relative error of at most 0.0045.
Values may be sent and summed in bfloat16 or wider, within the bound.
A program may use at most 128 MiB of HBM per device.

```python
import jax
import jax.numpy as jnp
from jax import lax

D = 1024
H = 4096
NACT = 256
A = 16
S_DEV = 32
BUF_DEV = 256
ENS = 16
STATES = 64
N_BATCH = 2


def touch_ends(array, key, least, high):
    index_at = [jax.random.randint(jax.random.fold_in(key, axis), (), 0, length) for axis, length in enumerate(array.shape)]
    longest = array.shape.index(max(array.shape))
    next_to = index_at[:longest] + [(index_at[longest] + 1) % array.shape[longest]] + index_at[longest + 1:]
    return array.at[tuple(index_at)].set(least).at[tuple(next_to)].set(high)


def shard_levels(own_key, shape, shards, least, top_value):
    factor_of, own = 1.0, jax.random.fold_in(own_key, 6)
    for axis_at, shards_of in shards:
        steps = jnp.exp(jax.random.uniform(jax.random.fold_in(own, axis_at), (shards_of,), jnp.float32, least / len(shards), top_value / len(shards)))
        factor_of = factor_of * jnp.repeat(steps, shape[axis_at] // shards_of).reshape([-1 if axis == axis_at else 1 for axis in range(len(shape))])
    return factor_of


def scatter_about(stream_key, extent, deviation, bound, pieces=(), kind=jnp.bfloat16):
    array = jax.random.normal(stream_key, extent, jnp.float32) * deviation
    if len(pieces) > 0:
        array = shard_levels(stream_key, extent, pieces, -0.22, 0.18) * array
    return jnp.clip(array, min=-bound, max=bound).astype(kind)


def setup_inputs(seed: int = 0) -> dict:
    key_list = jax.random.split(jax.random.key(seed), 12)
    return {
        "replay_obs": scatter_about(key_list[0], (N_BATCH * BUF_DEV, D), 0.7, 4.1875, ((0, 2),)),
        "replay_next": scatter_about(key_list[1], (N_BATCH * BUF_DEV, D), 0.7, 4.1875, ((0, 2),)),
        "batch_rows": touch_ends(jax.random.randint(key_list[2], (STATES,), 0, BUF_DEV), jax.random.fold_in(key_list[2], 1), 0, BUF_DEV - 1).astype(jnp.int32),
        "data_action": touch_ends(jax.random.randint(key_list[3], (STATES,), 0, NACT), jax.random.fold_in(key_list[3], 1), 0, NACT - 1).astype(jnp.int32),
        "next_action": touch_ends(jax.random.randint(key_list[4], (STATES,), 0, NACT), jax.random.fold_in(key_list[4], 1), 0, NACT - 1).astype(jnp.int32),
        "sampled_actions": touch_ends(jax.random.randint(key_list[5], (STATES, A), 0, NACT), jax.random.fold_in(key_list[5], 1), 0, NACT - 1).astype(jnp.int32),
        "reward": scatter_about(key_list[6], (STATES,), 1.0, 6.0, ((0, 2),), jnp.float32),
        "next_logp": jnp.clip(-6.0 + 8.0 * jax.random.uniform(key_list[7], (STATES,), jnp.float32) ** shard_levels(key_list[7], (STATES,), ((0, 2),), -0.2, 0.2), -6.0, 2.0),
        "action_table": scatter_about(key_list[8], (NACT, D), 0.7, 4.1875),
        "w1": scatter_about(key_list[9], (ENS, H, D), D ** -0.5, 0.1875, ((0, 16),)),
        "w2": scatter_about(key_list[10], (ENS, H), (4.0 / H ** 0.5), 0.375, ((0, 16),), jnp.float32),
    }


discount = 0.99
entropy_temp = 0.2
penalty_weight = 1.0
diversity_weight = 1000.0

def silu_terms(preact):
    sigmoid_v = jax.nn.sigmoid(preact)
    silu_out = preact * sigmoid_v
    slope_one = sigmoid_v * (1.0 + preact * (1.0 - sigmoid_v))
    return (silu_out, slope_one, sigmoid_v)

def reference(replay_obs, replay_next, batch_rows, data_action, next_action, sampled_actions, reward, next_logp, action_table, w1, w2):
    owners = jnp.arange(STATES, dtype=jnp.int32) // S_DEV
    row_ids = owners * BUF_DEV + batch_rows.astype(jnp.int32)
    obs_rows = jnp.take(replay_obs, row_ids, axis=0).astype(jnp.float32)
    next_rows = jnp.take(replay_next, row_ids, axis=0).astype(jnp.float32)
    table_f = action_table.astype(jnp.float32)
    x_next = (next_rows + jnp.take(table_f, next_action, axis=0)).astype(jnp.bfloat16)
    x_data = (obs_rows + jnp.take(table_f, data_action, axis=0)).astype(jnp.bfloat16)
    x_samp = (obs_rows[:, None, :] + jnp.take(table_f, sampled_actions, axis=0)).astype(jnp.bfloat16)
    x_samp = x_samp.reshape(STATES * A, D)

    def data_pass(weight, readout):
        preact = jnp.dot(x_data, weight.T, preferred_element_type=jnp.float32)
        silu_out, slope_one, sigmoid_v = silu_terms(preact)
        coeffs = (readout * slope_one).astype(jnp.bfloat16)
        grad_in = jnp.dot(coeffs, weight, preferred_element_type=jnp.float32)
        in_norm = jnp.sqrt(lax.optimization_barrier(jnp.sum(grad_in * grad_in, axis=-1, keepdims=True)) + 1.0)
        return (preact, silu_out, slope_one, sigmoid_v, coeffs, in_norm, grad_in / in_norm)

    def forward(params):
        weight, readout = params
        pre_next = jnp.dot(x_next, weight.T, preferred_element_type=jnp.float32)
        q_next = lax.optimization_barrier(jnp.sum(silu_terms(pre_next)[0] * readout, axis=-1))
        unit_dir = data_pass(weight, readout)[6]
        return (q_next, unit_dir)
    q_next_all, units = lax.map(forward, (w1, w2))
    target_floor = lax.optimization_barrier(jnp.min(q_next_all, axis=0))
    target = reward + discount * (target_floor - entropy_temp * next_logp)
    spread = lax.optimization_barrier(jnp.sum(units, axis=0))

    def backward(params):
        weight, readout = params
        preact, silu_out, slope_one, sigmoid_v, coeffs, in_norm, unit_dir = data_pass(weight, readout)
        q_data = lax.optimization_barrier(jnp.sum(silu_out * readout, axis=-1))
        pre_samp = jnp.dot(x_samp, weight.T, preferred_element_type=jnp.float32)
        silu_samp, slope_samp, _ = silu_terms(pre_samp)
        q_samp = lax.optimization_barrier(jnp.sum(silu_samp * readout, axis=-1)).reshape(STATES, A)
        td_gap = q_data - target
        log_mass = jnp.log(lax.optimization_barrier(jnp.sum(jnp.exp(q_samp), axis=-1)))
        action_prob = jnp.exp(q_samp - log_mass[:, None])
        div_row = lax.optimization_barrier(jnp.sum(unit_dir * (spread - unit_dir), axis=-1))
        stats = jnp.stack([jnp.sum(td_gap * td_gap), jnp.sum(log_mass - q_data), jnp.sum(div_row)]) / STATES
        dq_data = (2.0 * td_gap - penalty_weight) / STATES
        dq_samp = (penalty_weight * action_prob / STATES).reshape(STATES * A)
        dunit = 2.0 * diversity_weight / (ENS - 1) / STATES * (spread - unit_dir)
        dgrad = ((dunit - unit_dir * lax.optimization_barrier(jnp.sum(unit_dir * dunit, axis=-1, keepdims=True))) / in_norm).astype(jnp.bfloat16)
        dcoef = jnp.dot(dgrad, weight.T, preferred_element_type=jnp.float32)
        curve_two = sigmoid_v * (1.0 - sigmoid_v) * (2.0 + preact * (1.0 - 2.0 * sigmoid_v))
        dpre_data = (dq_data[:, None] * readout * slope_one + dcoef * readout * curve_two).astype(jnp.bfloat16)
        dpre_samp = (dq_samp[:, None] * readout * slope_samp).astype(jnp.bfloat16)
        grad_v = lax.optimization_barrier(jnp.sum(dq_data[:, None] * silu_out, axis=0)) + lax.optimization_barrier(jnp.sum(dq_samp[:, None] * silu_samp, axis=0)) + lax.optimization_barrier(jnp.sum(dcoef * slope_one, axis=0))
        grad_w = jnp.dot(dpre_data.T, x_data, preferred_element_type=jnp.float32)
        grad_w = grad_w + jnp.dot(dpre_samp.T, x_samp, preferred_element_type=jnp.float32)
        grad_w = grad_w + jnp.dot(coeffs.T, dgrad, preferred_element_type=jnp.float32)
        return (grad_w, grad_v, stats)
    grad_w1, grad_w2, critic_stats = lax.map(backward, (w1, w2))
    return (grad_w1, grad_w2, critic_stats)
```

```python
import functools

import jax
import jax.numpy as jnp
from jax import lax
from jax.experimental import pallas as pl
from jax.experimental.pallas import tpu as pltpu
from jax.sharding import PartitionSpec as P

discount = 0.99
entropy_temp = 0.2
penalty_weight = 1.0
diversity_weight = 1000.0

MESH = pl.DeviceIdType.MESH
F32 = jnp.float32
BF16 = jnp.bfloat16
CHUNK = 256
LANES = 128


def dot_t(a, b):
    return lax.dot_general(a, b, (((1,), (1,)), ((), ())), preferred_element_type=F32)


def sigmoid(x):
    return 0.5 * jnp.tanh(0.5 * x) + 0.5


def kernel(
    n_ens, per_dev, samples, critics_total,
    obs_ref, next_ref, rows_ref, acts_ref, aux_ref, table_ref, w2_ref, w1_ref,
    lhs_ref, rhs_ref, gv_ref, stat_ref,
    wbuf, xall, acts_in, aux_in, sel, sel_dq, ptab, pbuf, base, pre0, vb, sbuf, ubuf,
    gpart, gsend, grecv, qpart, qrecv, unit, usend, urecv, qmine, qall, spread_mine, spread_all,
    dgrad, div_out, div_in, gsamp, gvsamp, gvbuf,
    w_sem, a_send, a_recv, g_send, g_recv, u_send, u_recv, m_send, m_recv, s_send, s_recv,
    d_send, d_recv, v_send, v_recv,
):
    e = lax.axis_index("ens")
    b = lax.axis_index("batch")
    peer = 1 - b
    states = 2 * per_dev
    block = 2 * states
    nact = table_ref.shape[0]
    width = table_ref.shape[1]
    cols = acts_ref.shape[1]
    half = wbuf.shape[0]
    chunks = half // CHUNK
    pair = {"ens": e, "batch": peer}

    def other(k):
        return {"ens": lax.rem(e + k, n_ens), "batch": b}

    barrier = pltpu.get_barrier_semaphore()
    pl.semaphore_signal(barrier, inc=1, device_id=pair, device_id_type=MESH)

    def greet(k, carry):
        pl.semaphore_signal(barrier, inc=1, device_id=other(k), device_id_type=MESH)
        return carry

    lax.fori_loop(1, n_ens, greet, 0)

    def w_copy(c):
        return pltpu.make_async_copy(
            w1_ref.at[0, pl.ds(b * half + c * CHUNK, CHUNK), :],
            wbuf.at[pl.ds(c * CHUNK, CHUNK), :],
            w_sem.at[c],
        )

    for c in range(chunks):
        w_copy(c).start()

    own_rows = pl.ds(pl.multiple_of(b * per_dev, per_dev), per_dev)
    peer_rows = pl.ds(pl.multiple_of(peer * per_dev, per_dev), per_dev)
    pick = rows_ref[...] == lax.broadcasted_iota(jnp.int32, (per_dev, obs_ref.shape[0]), 1)
    pick = jnp.where(pick, 1.0, 0.0).astype(BF16)
    xall[0, own_rows, :] = jnp.dot(pick, next_ref[...], preferred_element_type=F32).astype(BF16)
    xall[1, own_rows, :] = jnp.dot(pick, obs_ref[...], preferred_element_type=F32).astype(BF16)
    pl.semaphore_wait(barrier, n_ens)

    def remote(src, dst, send, recv, to):
        return pltpu.make_async_remote_copy(
            src_ref=src, dst_ref=dst, send_sem=send, recv_sem=recv,
            device_id=to, device_id_type=MESH,
        )

    first = [
        remote(xall.at[:, own_rows, :], xall.at[:, own_rows, :], a_send.at[0], a_recv.at[0], pair),
        remote(acts_ref, acts_in, a_send.at[1], a_recv.at[1], pair),
        remote(aux_ref, aux_in, a_send.at[2], a_recv.at[2], pair),
    ]
    for copy in first:
        copy.start()

    def table_step(c, carry):
        rows = pl.ds(pl.multiple_of(c * CHUNK, CHUNK), CHUNK)
        w_copy(c).wait()
        ptab[rows, :] = dot_t(wbuf[rows, :], table_ref[...]).astype(BF16)
        v_row = w2_ref[0:1, pl.ds(pl.multiple_of(b * half + c * CHUNK, CHUNK), CHUNK)]
        vb[rows, :] = jnp.transpose(jnp.broadcast_to(v_row, (LANES, CHUNK)))
        return carry

    lax.fori_loop(0, chunks, table_step, 0)

    for copy in first:
        copy.wait()
    acts = acts_ref[...] + acts_in[...]
    lane_all = lax.broadcasted_iota(jnp.int32, (1, cols), 1)
    state_row = jnp.where(lane_all >= states, nact + lax.rem(lane_all, states), -1)
    for j in range(cols // LANES):
        at = slice(j * LANES, (j + 1) * LANES)
        row = lax.broadcasted_iota(jnp.int32, (nact + block, LANES), 0)
        hit = jnp.logical_or(row == acts[:, at], row == state_row[:, at])
        sel[:, at] = jnp.where(hit, 1.0, 0.0).astype(BF16)

    lane = lax.broadcasted_iota(jnp.int32, (1, block), 1)
    low = lane < states
    gpart[...] = jnp.zeros_like(gpart)
    SUB = 32

    def forward_step(c, q_acc):
        rows = pl.ds(pl.multiple_of(c * CHUNK, CHUNK), CHUNK)
        w = wbuf[rows, :]
        x = jnp.concatenate([xall[0], xall[1]], axis=0)
        p0 = dot_t(w, x)
        pbuf[...] = jnp.dot(ptab[rows, :], sel[:nact, :], preferred_element_type=F32)
        pre0[rows, :] = p0 + pbuf[:, :block]
        base[...] = jnp.where(low, pltpu.roll(p0, states, 1), p0)

        def sub_step(r, acc):
            here = pl.ds(pl.multiple_of(r * SUB, SUB), SUB)
            there = pl.ds(pl.multiple_of(c * CHUNK + r * SUB, SUB), SUB)
            v = vb[there, :]
            out = []
            for j in range(cols // LANES):
                at = slice(j * LANES, (j + 1) * LANES)
                if j == 0:
                    pre = pre0[there, :]
                else:
                    pre = pbuf[here, at] + base[here, :]
                sig = sigmoid(pre)
                silu = pre * sig
                slope = sig * (1.0 + (pre - silu))
                vs = v * slope
                if j == 0:
                    base_c[here, :] = vs
                else:
                    dst = slice((j - 1) * LANES, j * LANES)
                    sbuf[there, dst] = vs.astype(BF16)
                    ubuf[there, dst] = silu.astype(BF16)
                sv = silu * v
                part = sv[0:8]
                for t in range(1, SUB // 8):
                    part = part + sv[8 * t:8 * t + 8]
                out.append(acc[j] + part)
            return tuple(out)

        base_c = pbuf.at[:, :block]
        q_acc = lax.fori_loop(0, CHUNK // SUB, sub_step, q_acc)
        co = jnp.transpose(pbuf[:, :block])[states:, :].astype(BF16)
        gpart[...] += jnp.dot(co, w, preferred_element_type=F32)
        return q_acc

    zero = jnp.zeros((8, LANES), F32)
    q_acc = lax.fori_loop(0, chunks, forward_step, (zero,) * (cols // LANES))
    for j in range(cols // LANES):
        qpart[:, j * LANES:(j + 1) * LANES] = jnp.sum(q_acc[j], axis=0, keepdims=True)
    gsend[...] = gpart[peer_rows, :].astype(gsend.dtype)
    second = [
        remote(qpart, qrecv, g_send.at[0], g_recv.at[0], pair),
        remote(gsend, grecv, g_send.at[1], g_recv.at[1], pair),
    ]
    for copy in second:
        copy.start()
    second[0].wait()
    q = qpart[...] + qrecv[...]
    q0 = q[:, :block]
    qmine[...] = jnp.broadcast_to(q0, qmine.shape)

    def q_copy(k):
        return remote(qmine, qall.at[k], m_send.at[k], m_recv.at[k], other(k))

    def u_copy(k):
        return remote(
            usend.at[lax.rem(e + k, n_ens)], urecv.at[k], u_send.at[k], u_recv.at[k], other(k)
        )

    def s_copy(k):
        return remote(spread_mine, spread_all.at[e], s_send.at[k], s_recv.at[k], other(k))

    def start_all(make):
        def go(k, carry):
            make(k).start()
            return carry
        lax.fori_loop(1, n_ens, go, 0)

    def wait_all(make):
        def go(k, carry):
            make(k).wait()
            return carry
        lax.fori_loop(1, n_ens, go, 0)

    start_all(q_copy)
    second[1].wait()
    grad_in = gpart[own_rows, :] + grecv[...].astype(F32)
    norm_sq = jnp.sum(grad_in * grad_in, axis=-1, keepdims=True) + 1.0
    in_norm = jnp.sqrt(norm_sq)
    unit[...] = grad_in / in_norm
    piece = usend.shape[1]
    per_col = per_dev // piece
    for p in range(n_ens):
        c0, r0 = p // per_col, (p % per_col) * piece
        usend[p] = unit[r0:r0 + piece, c0 * LANES:(c0 + 1) * LANES].astype(BF16)
    start_all(u_copy)

    exps = jnp.exp(q[:, block:])
    mass = exps[:, :block]
    for j in range(1, (cols - block) // block):
        mass = mass + exps[:, j * block:(j + 1) * block]
    mass = mass + pltpu.roll(mass, states, 1)
    log_mass = jnp.log(mass)
    tiled = jnp.concatenate([log_mass] * ((cols - block) // block), axis=1)
    dq_samp = penalty_weight * jnp.exp(q[:, block:] - tiled) / states
    for j in range((cols - block) // LANES):
        at = slice(j * LANES, (j + 1) * LANES)
        src = slice(block + j * LANES, block + (j + 1) * LANES)
        sel_dq[:, at] = (sel[:, src].astype(F32) * dq_samp[:, at]).astype(BF16)

    def samp_step(c, carry):
        rows = pl.ds(pl.multiple_of(c * CHUNK, CHUNK), CHUNK)
        gsamp[rows, :] = dot_t(sbuf[rows, :], sel_dq[...])

        def sub_step(r, inner):
            there = pl.ds(pl.multiple_of(c * CHUNK + r * SUB, SUB), SUB)
            total = ubuf[there, :LANES].astype(F32) * dq_samp[:, :LANES]
            for j in range(1, (cols - block) // LANES):
                at = slice(j * LANES, (j + 1) * LANES)
                total = total + ubuf[there, at].astype(F32) * dq_samp[:, at]
            gvsamp[there, :] = total
            return inner

        lax.fori_loop(0, CHUNK // SUB, sub_step, 0)
        return carry

    middle = chunks // 2
    lax.fori_loop(0, middle, samp_step, 0)

    wait_all(u_copy)
    total = usend[e].astype(F32)
    for k in range(1, n_ens):
        total = total + urecv[k].astype(F32)
    spread_mine[...] = total.astype(BF16)
    spread_all[e] = total.astype(BF16)
    start_all(s_copy)
    lax.fori_loop(middle, chunks, samp_step, 0)
    wait_all(q_copy)
    floor = qmine[...]
    for k in range(1, n_ens):
        floor = jnp.minimum(floor, qall[k])
    floor = pltpu.roll(floor, states, 1)[0:1, :]
    aux = aux_ref[...] + aux_in[...]
    target = aux[0:1, :] + discount * (floor - entropy_temp * aux[1:2, :])
    td_gap = q0 - target
    dq_data = jnp.where(low, 0.0, (2.0 * td_gap - penalty_weight) / states)

    wait_all(s_copy)
    scale = 2.0 * diversity_weight / (critics_total - 1) / states
    for p in range(n_ens):
        c0, r0 = p // per_col, (p % per_col) * piece
        gpart[r0:r0 + piece, c0 * LANES:(c0 + 1) * LANES] = spread_all[p].astype(F32)
    unit_dir = unit[...]
    away = gpart[:per_dev, :] - unit_dir
    div_row = jnp.sum(unit_dir * away, axis=-1, keepdims=True)
    dg = scale * (away - unit_dir * div_row) / in_norm
    dg_rows = pl.ds(pl.multiple_of(states + b * per_dev, per_dev), per_dev)
    dgrad[:states, :] = jnp.zeros((states, width), BF16)
    dgrad[dg_rows, :] = dg.astype(BF16)
    div_sum = jnp.sum(div_row, axis=0, keepdims=True)
    div_out[...] = jnp.broadcast_to(div_sum, div_out.shape)
    third = [
        remote(dgrad.at[dg_rows, :], dgrad.at[dg_rows, :], d_send.at[0], d_recv.at[0], pair),
        remote(div_out, div_in, d_send.at[1], d_recv.at[1], pair),
    ]
    for copy in third:
        copy.start()
    rhs_ref[:nact, :] = table_ref[...]
    rhs_ref[nact:nact + states, :] = xall[1]
    for copy in third:
        copy.wait()
    rhs_ref[nact + states:, :] = dgrad[states:, :]

    td_total = jnp.sum(jnp.where(low, 0.0, td_gap * td_gap), axis=1, keepdims=True)
    gap_total = jnp.sum(jnp.where(low, 0.0, log_mass - q0), axis=1, keepdims=True)
    div_total = div_out[0:1, :] + div_in[0:1, :]
    stats = jnp.where(lane == 0, td_total, jnp.where(lane == 1, gap_total, div_total))
    stat_ref[...] = stats / states

    def data_step(c, carry):
        rows = pl.ds(pl.multiple_of(c * CHUNK, CHUNK), CHUNK)
        dcoef = dot_t(wbuf[rows, :], dgrad[...])
        pre = pre0[rows, :]
        v = vb[rows, :]
        sig = sigmoid(pre)
        silu = pre * sig
        slope = sig * (1.0 + (pre - silu))
        curve = sig * (1.0 - sig) * (2.0 + pre * (1.0 - 2.0 * sig))
        dpre = (v * (dq_data * slope + dcoef * curve)).astype(BF16)
        coeff = jnp.where(low, 0.0, v * slope)
        grads = gsamp[rows, :] + dot_t(dpre, sel[:, :block])
        lhs_ref[rows, :nact] = grads[:, :nact].astype(BF16)
        lhs_ref[rows, nact:] = (grads[:, nact:] + coeff).astype(BF16)
        gv = gvsamp[rows, :] + dq_data * silu + dcoef * slope
        gvbuf[b, pl.ds(c, 1), :] = jnp.sum(jnp.transpose(gv), axis=0, keepdims=True)
        return carry

    lax.fori_loop(0, chunks, data_step, 0)
    last = remote(gvbuf.at[b], gvbuf.at[b], v_send, v_recv, pair)
    last.start()
    last.wait()
    gv_ref[...] = gvbuf[...]


def body(
    replay_obs, replay_next, batch_rows, data_action, next_action, sampled_actions,
    reward, next_logp, action_table, w1, w2,
):
    per_dev = batch_rows.shape[0]
    samples = sampled_actions.shape[1]
    width = replay_obs.shape[1]
    hidden = w1.shape[1]
    n_batch = lax.axis_size("batch")
    n_ens = lax.axis_size("ens")
    if n_batch != 2 or w1.shape[0] != 1:
        raise ValueError("unsupported mesh")
    states = per_dev * n_batch
    block = 2 * states
    half = hidden // n_batch
    nact = action_table.shape[0]
    cols = (samples + 2) * states
    chunks = half // CHUNK
    piece = per_dev * width // LANES // n_ens
    mine = jnp.arange(n_batch) == lax.axis_index("batch")
    acts = jnp.concatenate([next_action[None], data_action[None], sampled_actions.T], axis=0)
    acts = jnp.where(mine[None, :, None], acts[:, None, :], 0).reshape(1, cols)
    aux = jnp.stack([reward, next_logp])
    aux = jnp.where(mine[None, :, None], aux[:, None, :], 0.0).reshape(2, states)
    aux = jnp.concatenate([jnp.zeros_like(aux), aux], axis=1)
    vmem = pl.BlockSpec(memory_space=pltpu.VMEM)
    dma = pltpu.SemaphoreType.DMA
    lhs, rhs, gv, stats = pl.pallas_call(
        functools.partial(kernel, n_ens, per_dev, samples, n_ens * w1.shape[0]),
        out_shape=(
            jax.ShapeDtypeStruct((half, nact + block), BF16),
            jax.ShapeDtypeStruct((nact + block, width), BF16),
            jax.ShapeDtypeStruct((2, chunks, CHUNK), F32),
            jax.ShapeDtypeStruct((1, block), F32),
        ),
        in_specs=[vmem] * 7 + [pl.BlockSpec(memory_space=pl.ANY)],
        out_specs=(vmem,) * 4,
        scratch_shapes=[
            pltpu.VMEM((half, width), BF16),
            pltpu.VMEM((2, states, width), BF16),
            pltpu.VMEM((1, cols), jnp.int32),
            pltpu.VMEM((2, block), F32),
            pltpu.VMEM((nact + block, cols), BF16),
            pltpu.VMEM((nact + block, cols - block), BF16),
            pltpu.VMEM((half, nact), BF16),
            pltpu.VMEM((CHUNK, cols), F32),
            pltpu.VMEM((CHUNK, block), F32),
            pltpu.VMEM((half, block), F32),
            pltpu.VMEM((half, LANES), F32),
            pltpu.VMEM((half, cols - block), BF16),
            pltpu.VMEM((half, cols - block), BF16),
            pltpu.VMEM((states, width), F32),
            pltpu.VMEM((per_dev, width), BF16),
            pltpu.VMEM((per_dev, width), BF16),
            pltpu.VMEM((1, cols), F32),
            pltpu.VMEM((1, cols), F32),
            pltpu.VMEM((per_dev, width), F32),
            pltpu.VMEM((n_ens, piece, LANES), BF16),
            pltpu.VMEM((n_ens, piece, LANES), BF16),
            pltpu.VMEM((8, block), F32),
            pltpu.VMEM((n_ens, 8, block), F32),
            pltpu.VMEM((piece, LANES), BF16),
            pltpu.VMEM((n_ens, piece, LANES), BF16),
            pltpu.VMEM((block, width), BF16),
            pltpu.VMEM((8, block), F32),
            pltpu.VMEM((8, block), F32),
            pltpu.VMEM((half, nact + block), F32),
            pltpu.VMEM((half, LANES), F32),
            pltpu.VMEM((2, chunks, CHUNK), F32),
            dma((chunks,)),
            dma((3,)), dma((3,)), dma((2,)), dma((2,)),
            dma((n_ens,)), dma((n_ens,)), dma((n_ens,)), dma((n_ens,)), dma((n_ens,)), dma((n_ens,)),
            dma((2,)), dma((2,)), dma, dma,
        ],
        compiler_params=pltpu.CompilerParams(
            collective_id=0, has_side_effects=True, vmem_limit_bytes=60 * 1024 * 1024
        ),
    )(replay_obs, replay_next, batch_rows[:, None], acts, aux, action_table, w2, w1)
    grad_w1 = jnp.dot(lhs, rhs, preferred_element_type=F32)[None]
    return (grad_w1, gv.reshape(1, hidden), stats[:, :3])


def solution(mesh):
    return jax.shard_map(
        body,
        mesh=mesh,
        in_specs=(
            P("batch", None),
            P("batch", None),
            P("batch"),
            P("batch"),
            P("batch"),
            P("batch", None),
            P("batch"),
            P("batch"),
            P(),
            P("ens", None, None),
            P("ens", None),
        ),
        out_specs=(P("ens", "batch", None), P("ens", None), P("ens", None)),
        check_vma=False,
    )
```

```python
import functools

import jax
import jax.numpy as jnp
from jax import lax
from jax.experimental import pallas as pl
from jax.experimental.pallas import tpu as pltpu
from jax.sharding import PartitionSpec as P

discount = 0.99
entropy_temp = 0.2
penalty_weight = 1.0
diversity_weight = 1000.0

MESH = pl.DeviceIdType.MESH
F32 = jnp.float32
BF16 = jnp.bfloat16
CHUNK = 256
LANES = 128


def dot_t(a, b):
    return lax.dot_general(a, b, (((1,), (1,)), ((), ())), preferred_element_type=F32)


def sigmoid(x):
    return 0.5 * jnp.tanh(0.5 * x) + 0.5


def kernel(
    n_ens, per_dev, samples, critics_total,
    obs_ref, next_ref, rows_ref, next_act_ref, data_act_ref, samp_act_ref, reward_ref, logp_ref, table_ref, w2_ref, w1_ref,
    lhs_ref, rhs_ref, gv_ref, stat_ref,
    acts_ref, aux_ref, wbuf, xall, acts_in, aux_in, sel, sel_dq, ptab, pbuf, base, pre0, dbuf, cbuf, vb, sbuf, ubuf,
    gpart, gsend, grecv, qpart, qrecv, unit, usend, urecv, qmine, qall, spread_mine, spread_all,
    dgrad, div_out, div_in, gsamp, gvsamp, gvbuf,
    w_sem, a_send, a_recv, g_send, g_recv, u_send, u_recv, m_send, m_recv, s_send, s_recv,
    d_send, d_recv, v_send, v_recv,
):
    e = lax.axis_index("ens")
    b = lax.axis_index("batch")
    peer = 1 - b
    states = 2 * per_dev
    block = 2 * states
    nact = table_ref.shape[0]
    width = table_ref.shape[1]
    cols = acts_ref.shape[1]
    samp_cols = cols - block
    half = wbuf.shape[0]
    chunks = half // CHUNK
    pair = {"ens": e, "batch": peer}

    def other(k):
        return {"ens": lax.rem(e + k, n_ens), "batch": b}

    barrier = pltpu.get_barrier_semaphore()
    pl.semaphore_signal(barrier, inc=1, device_id=pair, device_id_type=MESH)

    def greet(k, carry):
        pl.semaphore_signal(barrier, inc=1, device_id=other(k), device_id_type=MESH)
        return carry

    lax.fori_loop(1, n_ens, greet, 0)

    def w_copy(c):
        return pltpu.make_async_copy(
            w1_ref.at[0, pl.ds(b * half + c * CHUNK, CHUNK), :],
            wbuf.at[pl.ds(c * CHUNK, CHUNK), :],
            w_sem.at[c],
        )

    for c in range(chunks):
        w_copy(c).start()

    own_rows = pl.ds(pl.multiple_of(b * per_dev, per_dev), per_dev)
    peer_rows = pl.ds(pl.multiple_of(peer * per_dev, per_dev), per_dev)
    buf_rows = obs_ref.shape[0]
    row = jnp.concatenate([rows_ref[...], jnp.zeros((1, LANES - per_dev), jnp.int32)], axis=1)
    pick = row == lax.broadcasted_iota(jnp.int32, (buf_rows, LANES), 0)
    pick = jnp.transpose(jnp.where(pick, 1.0, 0.0))[:per_dev, :].astype(BF16)
    xall[0, own_rows, :] = jnp.dot(pick, next_ref[...], preferred_element_type=F32).astype(BF16)
    xall[1, own_rows, :] = jnp.dot(pick, obs_ref[...], preferred_element_type=F32).astype(BF16)
    act_rows = [next_act_ref[...], data_act_ref[...]]
    act_rows += [samp_act_ref[i:i + 1, :] for i in range(samples)]

    def place(part):
        return [jnp.where(b == 0, part, jnp.zeros_like(part)), jnp.where(b == 0, jnp.zeros_like(part), part)]

    for j in range(cols // block):
        acts_ref[:, j * block:(j + 1) * block] = jnp.concatenate(
            place(act_rows[2 * j]) + place(act_rows[2 * j + 1]), axis=1
        )
    blank = jnp.zeros((1, states), F32)
    aux_ref[0:1, :] = jnp.concatenate([blank] + place(reward_ref[...]), axis=1)
    aux_ref[1:2, :] = jnp.concatenate([blank] + place(logp_ref[...]), axis=1)
    pl.semaphore_wait(barrier, n_ens)

    def remote(src, dst, send, recv, to):
        return pltpu.make_async_remote_copy(
            src_ref=src, dst_ref=dst, send_sem=send, recv_sem=recv,
            device_id=to, device_id_type=MESH,
        )

    first = [
        remote(xall.at[:, own_rows, :], xall.at[:, own_rows, :], a_send.at[0], a_recv.at[0], pair),
        remote(acts_ref, acts_in, a_send.at[1], a_recv.at[1], pair),
        remote(aux_ref, aux_in, a_send.at[2], a_recv.at[2], pair),
    ]
    for copy in first:
        copy.start()

    def table_step(c, carry):
        rows = pl.ds(pl.multiple_of(c * CHUNK, CHUNK), CHUNK)
        w_copy(c).wait()
        ptab[rows, :] = dot_t(wbuf[rows, :], table_ref[...]).astype(BF16)
        v_row = w2_ref[0:1, pl.ds(pl.multiple_of(b * half + c * CHUNK, CHUNK), CHUNK)]
        vb[rows, :] = jnp.transpose(jnp.broadcast_to(v_row, (LANES, CHUNK)))
        return carry

    lax.fori_loop(0, chunks, table_step, 0)

    for copy in first:
        copy.wait()
    acts = acts_ref[...] + acts_in[...]
    lane_all = lax.broadcasted_iota(jnp.int32, (1, cols), 1)
    state_row = jnp.where(lane_all >= states, nact + lax.rem(lane_all, states), -1)
    for j in range(cols // LANES):
        at = slice(j * LANES, (j + 1) * LANES)
        row = lax.broadcasted_iota(jnp.int32, (nact + block, LANES), 0)
        hit = jnp.logical_or(row == acts[:, at], row == state_row[:, at])
        sel[:, at] = jnp.where(hit, 1.0, 0.0).astype(BF16)

    lane = lax.broadcasted_iota(jnp.int32, (1, block), 1)
    low = lane < states
    gpart[...] = jnp.zeros_like(gpart)
    SUB = 32

    def data_forward(c, q_acc):
        rows = pl.ds(pl.multiple_of(c * CHUNK, CHUNK), CHUNK)
        w = wbuf[rows, :]
        x = jnp.concatenate([xall[0], xall[1]], axis=0)
        p0 = dot_t(w, x)
        pre = p0 + jnp.dot(ptab[rows, :], sel[:nact, :block], preferred_element_type=F32)
        pre0[rows, :] = pre
        base[rows, :] = jnp.where(low, pltpu.roll(p0, states, 1), p0)
        v = vb[rows, :]
        sig = sigmoid(pre)
        silu = pre * sig
        slope = sig * (1.0 + (pre - silu))
        co = jnp.transpose(v * slope)[states:, :].astype(BF16)
        gpart[...] += jnp.dot(co, w, preferred_element_type=F32)
        return q_acc + jnp.sum(silu * v, axis=0, keepdims=True)

    qpart[:, :block] = lax.fori_loop(0, chunks, data_forward, jnp.zeros((1, block), F32))
    gsend[...] = gpart[peer_rows, :].astype(gsend.dtype)
    second = [
        remote(qpart.at[:, :block], qrecv.at[:, :block], g_send.at[0], g_recv.at[0], pair),
        remote(gsend, grecv, g_send.at[1], g_recv.at[1], pair),
        remote(qpart.at[:, block:], qrecv.at[:, block:], g_send.at[2], g_recv.at[2], pair),
    ]
    second[0].start()
    second[1].start()

    def samp_forward(c, q_acc):
        rows = pl.ds(pl.multiple_of(c * CHUNK, CHUNK), CHUNK)
        pbuf[...] = jnp.dot(ptab[rows, :], sel[:nact, block:], preferred_element_type=F32)

        def sub_step(r, acc):
            here = pl.ds(pl.multiple_of(r * SUB, SUB), SUB)
            there = pl.ds(pl.multiple_of(c * CHUNK + r * SUB, SUB), SUB)
            v = vb[there, :]
            start = base[there, :]
            out = []
            for j in range(samp_cols // LANES):
                at = slice(j * LANES, (j + 1) * LANES)
                pre = pbuf[here, at] + start
                sig = sigmoid(pre)
                silu = pre * sig
                slope = sig * (1.0 + (pre - silu))
                sbuf[there, at] = (v * slope).astype(BF16)
                ubuf[there, at] = silu.astype(BF16)
                sv = silu * v
                part = sv[0:8]
                for t in range(1, SUB // 8):
                    part = part + sv[8 * t:8 * t + 8]
                out.append(acc[j] + part)
            return tuple(out)

        return lax.fori_loop(0, CHUNK // SUB, sub_step, q_acc)

    q_acc = (jnp.zeros((8, LANES), F32),) * (samp_cols // LANES)
    cut_one, cut_two = (3 * chunks) // 8, (6 * chunks) // 8
    q_acc = lax.fori_loop(0, cut_one, samp_forward, q_acc)
    second[0].wait()
    q0 = qpart[:, :block] + qrecv[:, :block]
    qmine[...] = jnp.broadcast_to(q0, qmine.shape)

    def q_copy(k):
        return remote(qmine, qall.at[k], m_send.at[k], m_recv.at[k], other(k))

    def u_copy(k):
        return remote(
            usend.at[lax.rem(e + k, n_ens)], urecv.at[k], u_send.at[k], u_recv.at[k], other(k)
        )

    def s_copy(k):
        return remote(spread_mine, spread_all.at[e], s_send.at[k], s_recv.at[k], other(k))

    def start_all(make):
        def go(k, carry):
            make(k).start()
            return carry
        lax.fori_loop(1, n_ens, go, 0)

    def wait_all(make):
        def go(k, carry):
            make(k).wait()
            return carry
        lax.fori_loop(1, n_ens, go, 0)

    start_all(q_copy)
    second[1].wait()
    grad_in = gpart[own_rows, :] + grecv[...].astype(F32)
    norm_sq = jnp.sum(grad_in * grad_in, axis=-1, keepdims=True) + 1.0
    in_norm = jnp.sqrt(norm_sq)
    unit[...] = grad_in / in_norm
    piece = usend.shape[1]
    per_col = per_dev // piece
    for p in range(n_ens):
        c0, r0 = p // per_col, (p % per_col) * piece
        usend[p] = unit[r0:r0 + piece, c0 * LANES:(c0 + 1) * LANES].astype(BF16)
    start_all(u_copy)

    q_acc = lax.fori_loop(cut_one, cut_two, samp_forward, q_acc)

    wait_all(u_copy)
    total = usend[e].astype(F32)
    for k in range(1, n_ens):
        total = total + urecv[k].astype(F32)
    spread_mine[...] = total.astype(BF16)
    spread_all[e] = total.astype(BF16)
    start_all(s_copy)
    q_acc = lax.fori_loop(cut_two, chunks, samp_forward, q_acc)
    for j in range(samp_cols // LANES):
        qpart[:, block + j * LANES:block + (j + 1) * LANES] = jnp.sum(q_acc[j], axis=0, keepdims=True)
    second[2].start()
    wait_all(q_copy)
    floor = qmine[...]
    for k in range(1, n_ens):
        floor = jnp.minimum(floor, qall[k])
    floor = pltpu.roll(floor, states, 1)[0:1, :]
    aux = aux_ref[...] + aux_in[...]
    target = aux[0:1, :] + discount * (floor - entropy_temp * aux[1:2, :])
    td_gap = q0 - target
    dq_data = jnp.where(low, 0.0, (2.0 * td_gap - penalty_weight) / states)

    wait_all(s_copy)
    scale = 2.0 * diversity_weight / (critics_total - 1) / states
    for p in range(n_ens):
        c0, r0 = p // per_col, (p % per_col) * piece
        gpart[r0:r0 + piece, c0 * LANES:(c0 + 1) * LANES] = spread_all[p].astype(F32)
    unit_dir = unit[...]
    away = gpart[:per_dev, :] - unit_dir
    div_row = jnp.sum(unit_dir * away, axis=-1, keepdims=True)
    dg = scale * (away - unit_dir * div_row) / in_norm
    dg_rows = pl.ds(pl.multiple_of(states + b * per_dev, per_dev), per_dev)
    dgrad[:states, :] = jnp.zeros((states, width), BF16)
    dgrad[dg_rows, :] = dg.astype(BF16)
    div_sum = jnp.sum(div_row, axis=0, keepdims=True)
    div_out[...] = jnp.broadcast_to(div_sum, div_out.shape)
    third = [
        remote(dgrad.at[dg_rows, :], dgrad.at[dg_rows, :], d_send.at[0], d_recv.at[0], pair),
        remote(div_out, div_in, d_send.at[1], d_recv.at[1], pair),
    ]
    for copy in third:
        copy.start()
    second[2].wait()
    q_samp = qpart[:, block:] + qrecv[:, block:]
    exps = jnp.exp(q_samp)
    mass = exps[:, :block]
    for j in range(1, (cols - block) // block):
        mass = mass + exps[:, j * block:(j + 1) * block]
    mass = mass + pltpu.roll(mass, states, 1)
    log_mass = jnp.log(mass)
    tiled = jnp.concatenate([log_mass] * ((cols - block) // block), axis=1)
    dq_samp = penalty_weight * jnp.exp(q_samp - tiled) / states
    for j in range((cols - block) // LANES):
        at = slice(j * LANES, (j + 1) * LANES)
        src = slice(block + j * LANES, block + (j + 1) * LANES)
        sel_dq[:, at] = (sel[:, src].astype(F32) * dq_samp[:, at]).astype(BF16)

    def samp_step(c, carry):
        rows = pl.ds(pl.multiple_of(c * CHUNK, CHUNK), CHUNK)
        gsamp[rows, :] = dot_t(sbuf[rows, :], sel_dq[...])

        def sub_step(r, inner):
            there = pl.ds(pl.multiple_of(c * CHUNK + r * SUB, SUB), SUB)
            total = ubuf[there, :LANES].astype(F32) * dq_samp[:, :LANES]
            for j in range(1, (cols - block) // LANES):
                at = slice(j * LANES, (j + 1) * LANES)
                total = total + ubuf[there, at].astype(F32) * dq_samp[:, at]
            gvsamp[there, :] = total
            return inner

        lax.fori_loop(0, CHUNK // SUB, sub_step, 0)
        return carry

    lax.fori_loop(0, chunks, samp_step, 0)
    rhs_ref[:nact, :] = table_ref[...]
    rhs_ref[nact:nact + states, :] = xall[1]
    for copy in third:
        copy.wait()
    rhs_ref[nact + states:, :] = dgrad[states:, :]

    td_total = jnp.sum(jnp.where(low, 0.0, td_gap * td_gap), axis=1, keepdims=True)
    gap_total = jnp.sum(jnp.where(low, 0.0, log_mass - q0), axis=1, keepdims=True)
    div_total = div_out[0:1, :] + div_in[0:1, :]
    stats = jnp.where(lane == 0, td_total, jnp.where(lane == 1, gap_total, div_total))
    stat_ref[...] = (stats / states)[:, :3]

    def data_step(c, carry):
        rows = pl.ds(pl.multiple_of(c * CHUNK, CHUNK), CHUNK)
        dcoef = dot_t(wbuf[rows, :], dgrad[...])
        pre = pre0[rows, :]
        v = vb[rows, :]
        sig = sigmoid(pre)
        silu = pre * sig
        slope = sig * (1.0 + (pre - silu))
        curve = sig * (1.0 - sig) * (2.0 + pre * (1.0 - 2.0 * sig))
        dpre = (v * (dq_data * slope + dcoef * curve)).astype(BF16)
        coeff = jnp.where(low, 0.0, v * slope)
        dbuf[rows, :] = dpre
        cbuf[rows, :] = coeff
        gv = gvsamp[rows, :] + dq_data * silu + dcoef * slope
        gvbuf[b, pl.ds(c, 1), :] = jnp.sum(jnp.transpose(gv), axis=0, keepdims=True)
        return carry

    lax.fori_loop(0, chunks, data_step, 0)
    last = remote(gvbuf.at[b], gvbuf.at[b], v_send, v_recv, pair)
    last.start()

    def out_step(c, carry):
        rows = pl.ds(pl.multiple_of(c * CHUNK, CHUNK), CHUNK)
        grads = gsamp[rows, :] + dot_t(dbuf[rows, :], sel[:, :block])
        lhs_ref[rows, :nact] = grads[:, :nact].astype(BF16)
        lhs_ref[rows, nact:] = (grads[:, nact:] + cbuf[rows, :]).astype(BF16)
        return carry

    lax.fori_loop(0, chunks, out_step, 0)
    last.wait()
    for i in range(2):
        for c in range(chunks):
            at = i * half + c * CHUNK
            gv_ref[:, at:at + CHUNK] = gvbuf[i, c:c + 1, :]


def body(
    replay_obs, replay_next, batch_rows, data_action, next_action, sampled_actions,
    reward, next_logp, action_table, w1, w2,
):
    per_dev = batch_rows.shape[0]
    samples = sampled_actions.shape[1]
    width = replay_obs.shape[1]
    hidden = w1.shape[1]
    n_batch = lax.axis_size("batch")
    n_ens = lax.axis_size("ens")
    if n_batch != 2 or w1.shape[0] != 1:
        raise ValueError("unsupported mesh")
    states = per_dev * n_batch
    block = 2 * states
    half = hidden // n_batch
    nact = action_table.shape[0]
    cols = (samples + 2) * states
    chunks = half // CHUNK
    piece = per_dev * width // LANES // n_ens
    vmem = pl.BlockSpec(memory_space=pltpu.VMEM)
    dma = pltpu.SemaphoreType.DMA
    lhs, rhs, gv, stats = pl.pallas_call(
        functools.partial(kernel, n_ens, per_dev, samples, n_ens * w1.shape[0]),
        out_shape=(
            jax.ShapeDtypeStruct((half, nact + block), BF16),
            jax.ShapeDtypeStruct((nact + block, width), BF16),
            jax.ShapeDtypeStruct((1, hidden), F32),
            jax.ShapeDtypeStruct((1, 3), F32),
        ),
        in_specs=[vmem] * 10 + [pl.BlockSpec(memory_space=pl.ANY)],
        out_specs=(vmem,) * 4,
        scratch_shapes=[
            pltpu.VMEM((1, cols), jnp.int32),
            pltpu.VMEM((2, block), F32),
            pltpu.VMEM((half, width), BF16),
            pltpu.VMEM((2, states, width), BF16),
            pltpu.VMEM((1, cols), jnp.int32),
            pltpu.VMEM((2, block), F32),
            pltpu.VMEM((nact + block, cols), BF16),
            pltpu.VMEM((nact + block, cols - block), BF16),
            pltpu.VMEM((half, nact), BF16),
            pltpu.VMEM((CHUNK, cols - block), F32),
            pltpu.VMEM((half, block), F32),
            pltpu.VMEM((half, block), F32),
            pltpu.VMEM((half, block), BF16),
            pltpu.VMEM((half, block), F32),
            pltpu.VMEM((half, LANES), F32),
            pltpu.VMEM((half, cols - block), BF16),
            pltpu.VMEM((half, cols - block), BF16),
            pltpu.VMEM((states, width), F32),
            pltpu.VMEM((per_dev, width), BF16),
            pltpu.VMEM((per_dev, width), BF16),
            pltpu.VMEM((1, cols), F32),
            pltpu.VMEM((1, cols), F32),
            pltpu.VMEM((per_dev, width), F32),
            pltpu.VMEM((n_ens, piece, LANES), BF16),
            pltpu.VMEM((n_ens, piece, LANES), BF16),
            pltpu.VMEM((8, block), F32),
            pltpu.VMEM((n_ens, 8, block), F32),
            pltpu.VMEM((piece, LANES), BF16),
            pltpu.VMEM((n_ens, piece, LANES), BF16),
            pltpu.VMEM((block, width), BF16),
            pltpu.VMEM((8, block), F32),
            pltpu.VMEM((8, block), F32),
            pltpu.VMEM((half, nact + block), F32),
            pltpu.VMEM((half, LANES), F32),
            pltpu.VMEM((2, chunks, CHUNK), F32),
            dma((chunks,)),
            dma((3,)), dma((3,)), dma((3,)), dma((3,)),
            dma((n_ens,)), dma((n_ens,)), dma((n_ens,)), dma((n_ens,)), dma((n_ens,)), dma((n_ens,)),
            dma((2,)), dma((2,)), dma, dma,
        ],
        compiler_params=pltpu.CompilerParams(
            collective_id=0, has_side_effects=True, vmem_limit_bytes=60 * 1024 * 1024
        ),
    )(
        replay_obs, replay_next, batch_rows[None], next_action[None], data_action[None],
        sampled_actions.T, reward[None], next_logp[None], action_table, w2, w1,
    )
    grad_w1 = jnp.dot(lhs, rhs, preferred_element_type=F32)[None]
    return (grad_w1, gv, stats)


def solution(mesh):
    return jax.shard_map(
        body,
        mesh=mesh,
        in_specs=(
            P("batch", None),
            P("batch", None),
            P("batch"),
            P("batch"),
            P("batch"),
            P("batch", None),
            P("batch"),
            P("batch"),
            P(),
            P("ens", None, None),
            P("ens", None),
        ),
        out_specs=(P("ens", "batch", None), P("ens", None), P("ens", None)),
        check_vma=False,
    )
```
